256 devices in a mesh: rep: 8 (over x_lo, y), tp: 8 (over z), fs: 4 (over x_hi, core).
Axes of the slice: x: 4 (x_hi: 2, x_lo: 2; x = x_hi * 2 + x_lo), y: 4, z: 8, core: 2. Of those that a mesh axis runs over, the one named last changes fastest.
Arguments:
- hidden: bfloat16 [64, 8192], P(('rep', 'fs'), 'tp'), may hold values from -6 to 6
- cache_key: bfloat16 [64, 2048, 1024], P(('rep', 'fs'), None, 'tp'), may hold values from -1300 to 1300
- cache_value: bfloat16 [64, 2048, 1024], P(('rep', 'fs'), None, 'tp'), may hold values from -6 to 6
- lengths: int32 [64], P(('rep', 'fs')), may hold values from 8 to 2047
- owner: int32 [1], replicated, may hold values from 0 to 32767
- query_weight: bfloat16 [8, 8192, 4096], P('rep', 'fs', 'tp'), may hold values from -0.0625 to 0.0625
- key_weight: bfloat16 [8, 8192, 1024], P('rep', 'fs', 'tp'), may hold values from -0.0625 to 0.0625
- value_weight: bfloat16 [8, 8192, 1024], P('rep', 'fs', 'tp'), may hold values from -0.0625 to 0.0625
- out_weight: bfloat16 [8, 4096, 8192], P('rep', 'tp', 'fs'), may hold values from -0.09375 to 0.09375
Outputs:
- mixed: bfloat16 [64, 8192], P(('rep', 'fs'), 'tp')
- new_key: bfloat16 [64, 1024], P(('rep', 'fs'), 'tp')
- new_value: bfloat16 [64, 1024], P(('rep', 'fs'), 'tp')
- fresh_query: bfloat16 [8, 8192, 4096], P('rep', 'fs', 'tp')
- fresh_key: bfloat16 [8, 8192, 1024], P('rep', 'fs', 'tp')
- fresh_value: bfloat16 [8, 8192, 1024], P('rep', 'fs', 'tp')
- fresh_out: bfloat16 [8, 4096, 8192], P('rep', 'tp', 'fs')
The draws below stay inside these ranges and needn't reach their ends.
Inputs may be any that keep to these rules, and one draw needn't show every extreme that they name: `lengths`: the number of positions already in each sequence's cache; the new token stands at that position.
All inputs are finite; a program needn't handle non-finite values.
Results may differ from the reference program's by a relative error of at most 0.0065.
Values may be sent and summed in bfloat16 or wider, within the bound.
No kernel may reach another device: no remote copies, remote signals or barrier semaphores. Data moves between devices by JAX's collectives and lax.ppermute only.
A program may use at most 64 MiB of HBM per device.

```python
import jax
import jax.numpy as jnp
from jax import lax

D = 8192
HQ = 32
KVH = 8
DH = 128
CACHE = 2048
BATCH = 64
N_REP = 8


def draw_cache_key(key, part):
    full_shape = (BATCH, CACHE, KVH * DH)
    noise_field = jnp.clip(jax.random.normal(key, full_shape, jnp.float32), -6.0, 6.0)
    return noise_field.astype(jnp.bfloat16)


def place_ends(array, stream_key, least, largest):
    longest = array.shape.index(max(array.shape))
    spots = []
    for shift in (0, 1):
        where = [jax.random.randint(jax.random.fold_in(stream_key, axis), (), 0, length) for axis, length in enumerate(array.shape)]
        where[longest] = (where[longest] + shift) % array.shape[longest]
        spots.append(tuple(where))
    return array.at[spots[0]].set(least).at[spots[1]].set(largest)


def levels(key, dims, cuts, least, largest):
    level = 1.0
    for dim, blocks in cuts:
        steps = jax.random.uniform(jax.random.fold_in(jax.random.fold_in(key, 6), dim), (blocks,), jnp.float32, least / len(cuts), largest / len(cuts))
        level = level * jnp.repeat(jnp.exp(steps), dims[dim] // blocks).reshape((-1,) + (1,) * (len(dims) - 1 - dim))
    return level


def noise(stream_key, extent, scale, limit, cuts=(), held_as=jnp.bfloat16):
    result = scale * jax.random.normal(stream_key, extent, jnp.float32)
    if cuts:
        result = result * levels(stream_key, extent, cuts, -0.22, 0.18)
    return jnp.clip(result, -limit, limit).astype(held_as)


def setup_inputs(seed: int = 0) -> dict:
    keys = jax.random.split(jax.random.key(seed), 10)
    hidden = noise(keys[0], (BATCH, D), 1.0, 6.0, ((0, 32), (1, 8)))
    cache_key = draw_cache_key(jax.random.fold_in(keys[9], 71), 0)
    cache_value = noise(keys[2], (BATCH, CACHE, KVH * DH), 1.0, 6.0, ((0, 32), (2, 8)))
    lengths = place_ends(jax.random.randint(keys[3], (BATCH,), 8, CACHE), jax.random.fold_in(keys[3], 1), 8, CACHE - 1).astype(jnp.int32)
    owner = jax.random.randint(keys[4], (1,), 0, N_REP * 4096).astype(jnp.int32)
    query_weight = noise(keys[5], (N_REP, D, HQ * DH), D ** -0.5, 0.0625, ((0, 8), (1, 4), (2, 8)))
    key_weight = noise(keys[6], (N_REP, D, KVH * DH), D ** -0.5, 0.0625, ((0, 8), (1, 4), (2, 8)))
    value_weight = noise(keys[7], (N_REP, D, KVH * DH), D ** -0.5, 0.0625, ((0, 8), (1, 4), (2, 8)))
    out_weight = noise(keys[8], (N_REP, HQ * DH, D), (HQ * DH) ** -0.5, 0.09375, ((0, 8), (1, 8), (2, 4)))
    return dict(hidden=hidden, cache_key=cache_key, cache_value=cache_value, lengths=lengths, owner=owner, query_weight=query_weight, key_weight=key_weight, value_weight=value_weight, out_weight=out_weight)


rope_base = 500000.0
epsilon = 1e-05

def rotate(heads, positions):
    half_dim = heads.shape[-1] // 2
    frequency = rope_base ** (-(jnp.arange(half_dim, dtype=jnp.float32) * 2.0 / heads.shape[-1]))
    angles = positions.astype(jnp.float32)[:, None] * frequency[None, :]
    cosine = jnp.cos(angles)[:, None, :]
    sine_part = jnp.sin(angles)[:, None, :]
    first_half = heads[..., :half_dim]
    second_half = heads[..., half_dim:]
    return jnp.concatenate([first_half * cosine - second_half * sine_part, second_half * cosine + first_half * sine_part], axis=-1)

def attend_one(items):
    query, own_key, own_value, keys_seq, values_seq, length = items
    scale = DH ** (-0.5)
    keys_wide = keys_seq.astype(jnp.float32).reshape(CACHE, KVH, DH)
    values_wide = values_seq.astype(jnp.float32).reshape(CACHE, KVH, DH)
    scores = jnp.einsum('hgd,thd->hgt', query, keys_wide) * scale
    own_score = jnp.einsum('hgd,hd->hg', query, own_key) * scale
    live = jnp.arange(CACHE, dtype=jnp.int32) < length
    masked = jnp.where(live, scores, -jnp.inf)
    row_max = jnp.maximum(lax.optimization_barrier(jnp.max(masked, axis=-1)), own_score)
    weights = jnp.where(live, jnp.exp(scores - row_max[..., None]), 0.0)
    own_weight = jnp.exp(own_score - row_max)
    denominator = lax.optimization_barrier(jnp.sum(weights, axis=-1)) + own_weight
    probs = lax.optimization_barrier((weights / denominator[..., None]).astype(jnp.bfloat16)).astype(jnp.float32)
    own_prob = lax.optimization_barrier((own_weight / denominator).astype(jnp.bfloat16)).astype(jnp.float32)
    context = jnp.einsum('hgt,thd->hgd', probs, values_wide)
    return context + own_prob[..., None] * own_value[:, None, :]

def reference(hidden, cache_key, cache_value, lengths, owner, query_weight, key_weight, value_weight, out_weight):
    owner_rank = (owner[0] % N_REP).astype(jnp.int32)
    query_block = lax.dynamic_index_in_dim(query_weight, owner_rank, 0, keepdims=False)
    key_block = lax.dynamic_index_in_dim(key_weight, owner_rank, 0, keepdims=False)
    value_block = lax.dynamic_index_in_dim(value_weight, owner_rank, 0, keepdims=False)
    out_block = lax.dynamic_index_in_dim(out_weight, owner_rank, 0, keepdims=False)
    hidden_wide = hidden.astype(jnp.float32)
    normed = (hidden_wide * lax.rsqrt(lax.optimization_barrier(jnp.mean(hidden_wide * hidden_wide, axis=-1, keepdims=True)) + epsilon)).astype(jnp.bfloat16)
    query_proj = jnp.dot(normed, query_block, preferred_element_type=jnp.float32)
    key_proj = jnp.dot(normed, key_block, preferred_element_type=jnp.float32)
    value_proj = jnp.dot(normed, value_block, preferred_element_type=jnp.float32)
    query_rot = rotate(query_proj.reshape(BATCH, HQ, DH), lengths).astype(jnp.bfloat16)
    key_new = rotate(key_proj.reshape(BATCH, KVH, DH), lengths).astype(jnp.bfloat16)
    value_new = value_proj.astype(jnp.bfloat16).reshape(BATCH, KVH, DH)
    group_size = HQ // KVH
    query_wide = lax.optimization_barrier(query_rot).astype(jnp.float32).reshape(BATCH, KVH, group_size, DH)
    key_wide = lax.optimization_barrier(key_new).astype(jnp.float32)
    value_wide = lax.optimization_barrier(value_new).astype(jnp.float32)
    context = lax.map(attend_one, (query_wide, key_wide, value_wide, cache_key, cache_value, lengths))
    context = context.astype(jnp.bfloat16).reshape(BATCH, HQ * DH)
    summed = jnp.dot(context, out_block, preferred_element_type=jnp.float32)
    mixed = (summed + hidden_wide).astype(jnp.bfloat16)
    fresh_query = jnp.broadcast_to(query_block[None], query_weight.shape)
    fresh_key = jnp.broadcast_to(key_block[None], key_weight.shape)
    fresh_value = jnp.broadcast_to(value_block[None], value_weight.shape)
    fresh_out = jnp.broadcast_to(out_block[None], out_weight.shape)
    return (mixed, key_new.reshape(BATCH, KVH * DH), value_new.reshape(BATCH, KVH * DH), fresh_query, fresh_key, fresh_value, fresh_out)
```

```python
import jax
import jax.numpy as jnp
from jax import lax
from jax.sharding import PartitionSpec as P

DH = 128


rope_base = 500000.0
epsilon = 1e-05


def from_root(shard, axis, root):
    mine = lax.axis_index(axis) == root
    return lax.psum(jnp.where(mine, shard, jnp.zeros_like(shard)), axis)


def cut_along(shard, dim, peers):
    lengths = shard.shape
    parts = shard.reshape(*lengths[:dim], peers, lengths[dim] // peers, *lengths[dim + 1 :])
    return jnp.moveaxis(parts, dim, 0)


def sent_and_summed(shard, axis, dim):
    peers = lax.axis_size(axis)
    parts = lax.all_to_all(cut_along(shard, dim, peers), axis, 0, 0, tiled=True)
    return jnp.sum(parts, axis=0)


def copy_for_each(shard, axis):
    peers = lax.axis_size(axis)
    return lax.all_to_all(
        jnp.broadcast_to(shard[None], (peers, *shard.shape)), axis, 0, 0, tiled=True
    )


def joined_along(parts, dim):
    parts = jnp.moveaxis(parts, 0, dim)
    lengths = parts.shape
    return parts.reshape(*lengths[:dim], lengths[dim] * lengths[dim + 1], *lengths[dim + 2 :])


def collect(shard, axis, dim):
    parts = copy_for_each(shard, axis)
    return joined_along(parts, dim)


def rotate(heads, positions):
    half_dim = heads.shape[-1] // 2
    frequency = rope_base ** (-(jnp.arange(half_dim, dtype=jnp.float32) * 2.0 / heads.shape[-1]))
    angles = positions.astype(jnp.float32)[:, None] * frequency[None, :]
    cosine = jnp.cos(angles)[:, None, :]
    sine_part = jnp.sin(angles)[:, None, :]
    first_half = heads[..., :half_dim]
    second_half = heads[..., half_dim:]
    return jnp.concatenate(
        [
            first_half * cosine - second_half * sine_part,
            second_half * cosine + first_half * sine_part,
        ],
        axis=-1,
    )


def attend(query, own_key, own_value, cache_key, cache_value, lengths):
    seqs, span, width = cache_key.shape
    kv_local = query.shape[1]
    head_size = query.shape[3]
    keys_view = cache_key.reshape(seqs, span, kv_local, head_size)
    values_view = cache_value.reshape(seqs, span, kv_local, head_size)
    scale = head_size ** (-0.5)
    scores = (
        jnp.einsum("shgd,sthd->shgt", query, keys_view, preferred_element_type=jnp.float32) * scale
    )
    own_score = (
        jnp.einsum("shgd,shd->shg", query, own_key, preferred_element_type=jnp.float32) * scale
    )
    live = (jnp.arange(span, dtype=jnp.int32)[None, :] < lengths[:, None])[:, None, None, :]
    masked = jnp.where(live, scores, -jnp.inf)
    row_max = jnp.maximum(jnp.max(masked, axis=-1), own_score)
    weights = jnp.where(live, jnp.exp(scores - row_max[..., None]), 0.0)
    own_weight = jnp.exp(own_score - row_max)
    denominator = jnp.sum(weights, axis=-1) + own_weight
    probs = (weights / denominator[..., None]).astype(jnp.bfloat16)
    own_prob = (own_weight / denominator).astype(jnp.bfloat16)
    context = jnp.einsum("shgt,sthd->shgd", probs, values_view, preferred_element_type=jnp.float32)
    return (
        context
        + own_prob.astype(jnp.float32)[..., None] * own_value.astype(jnp.float32)[:, :, None, :]
    )


def from_owner(parts, owner_rank):
    peers = lax.axis_size("rep")
    grouped = parts.reshape(peers, parts.shape[0] // peers, *parts.shape[1:])
    return lax.dynamic_index_in_dim(grouped, owner_rank, 0, keepdims=False)


def local(
    hidden,
    cache_key,
    cache_value,
    lengths,
    owner,
    query_weight,
    key_weight,
    value_weight,
    out_weight,
):
    reps, fss, tps = lax.axis_size("rep"), lax.axis_size("fs"), lax.axis_size("tp")
    owner_rank = owner[0] % reps
    fresh_query, fresh_key, fresh_value, fresh_out = (
        from_root(query_weight, "rep", owner_rank),
        from_root(key_weight, "rep", owner_rank),
        from_root(value_weight, "rep", owner_rank),
        from_root(out_weight, "rep", owner_rank),
    )
    seqs = hidden.shape[0]
    hidden_wide = collect(hidden, "tp", 1).astype(jnp.float32)
    normed = (
        hidden_wide
        * lax.rsqrt(jnp.mean(hidden_wide * hidden_wide, axis=-1, keepdims=True) + epsilon)
    ).astype(jnp.bfloat16)
    blocks = cut_along(normed, 1, fss)
    blocks = jnp.broadcast_to(blocks[None], (reps, *blocks.shape))
    blocks = blocks.reshape(reps * fss, *blocks.shape[2:])
    tokens = lax.all_to_all(blocks, ("rep", "fs"), 0, 0, tiled=True)
    tokens = tokens.reshape(reps * fss * seqs, tokens.shape[-1])
    query_width = query_weight.shape[2]
    key_width = key_weight.shape[2]
    partial = jnp.concatenate(
        [
            jnp.dot(tokens, query_weight[0], preferred_element_type=jnp.float32),
            jnp.dot(tokens, key_weight[0], preferred_element_type=jnp.float32),
            jnp.dot(tokens, value_weight[0], preferred_element_type=jnp.float32),
        ],
        axis=1,
    )
    partial = partial.reshape(reps * fss, seqs, partial.shape[1])
    shares = lax.all_to_all(partial, ("rep", "fs"), 0, 0, tiled=True)
    joined = jnp.sum(from_owner(shares, owner_rank), axis=0)
    query_proj = joined[:, :query_width]
    key_proj = joined[:, query_width : query_width + key_width]
    value_proj = joined[:, query_width + key_width :]
    q_heads = query_proj.shape[1] // DH
    kv_heads = key_proj.shape[1] // DH
    query_rot = rotate(query_proj.reshape(seqs, q_heads, DH), lengths).astype(jnp.bfloat16)
    query_rot = query_rot.reshape(seqs, kv_heads, q_heads // kv_heads, DH)
    key_new = rotate(key_proj.reshape(seqs, kv_heads, DH), lengths).astype(jnp.bfloat16)
    value_new = value_proj.astype(jnp.bfloat16).reshape(seqs, kv_heads, DH)
    context = attend(query_rot, key_new, value_new, cache_key, cache_value, lengths)
    context = context.astype(jnp.bfloat16).reshape(seqs, q_heads * DH)
    contexts = lax.all_to_all(
        jnp.broadcast_to(context[None], (reps * fss, *context.shape)), ("rep", "fs"), 0, 0, tiled=True
    ).reshape(reps * fss * seqs, q_heads * DH)
    partial_out = jnp.dot(contexts, out_weight[0], preferred_element_type=jnp.float32)
    partial_out = partial_out.reshape(reps * fss, seqs, partial_out.shape[1])
    terms = lax.all_to_all(partial_out, ("rep", "fs"), 0, 0, tiled=True)
    terms = joined_along(from_owner(terms, owner_rank), 1)
    summed = sent_and_summed(terms, "tp", 1)
    mixed = (summed + hidden.astype(jnp.float32)).astype(jnp.bfloat16)
    return (
        mixed,
        key_new.reshape(seqs, kv_heads * DH),
        value_new.reshape(seqs, kv_heads * DH),
        fresh_query,
        fresh_key,
        fresh_value,
        fresh_out,
    )


def solution(mesh):
    return jax.shard_map(
        local,
        mesh=mesh,
        in_specs=(
            P(("rep", "fs"), "tp"),
            P(("rep", "fs"), None, "tp"),
            P(("rep", "fs"), None, "tp"),
            P(("rep", "fs")),
            P(),
            P("rep", "fs", "tp"),
            P("rep", "fs", "tp"),
            P("rep", "fs", "tp"),
            P("rep", "tp", "fs"),
        ),
        out_specs=(
            P(("rep", "fs"), "tp"),
            P(("rep", "fs"), "tp"),
            P(("rep", "fs"), "tp"),
            P("rep", "fs", "tp"),
            P("rep", "fs", "tp"),
            P("rep", "fs", "tp"),
            P("rep", "tp", "fs"),
        ),
        check_vma=False,
    )
```

```python
import jax
import jax.numpy as jnp
import numpy as np
from jax import lax
from jax.experimental import pallas as pl
from jax.experimental.pallas import tpu as pltpu
from jax.sharding import PartitionSpec as P

DH = 128


rope_base = 500000.0
epsilon = 1e-05


FLIPS = (4, 1, 3)
WIDTH = 512
PIECE = 32
PIECES = 14
CHUNKS = 4
TOTAL = 5120 // PIECE
ROWS = PIECE * PIECES
ROUNDS = CHUNKS + 3
PER_BLOCK = 512 // PIECE
GRANT = 8 * 1024 * 1024
IN_VMEM = pl.BlockSpec(memory_space=pltpu.VMEM)
IN_HBM = pl.BlockSpec(memory_space=pltpu.HBM)
IN_SMEM = pl.BlockSpec(memory_space=pltpu.SMEM)
TREE = {1: 0, 3: 1, 5: 2, 2: 0, 4: 0, 7: 2, 6: 0}


def rotated(corner, turns):
    for _ in range(turns % 3):
        corner = ((corner << 1) & 7) | (corner >> 2)
    return corner


def came_by(tree, corner):
    return (TREE[rotated(corner, 3 - tree)] + tree) % 3


def plan():
    table = [[0, 0, 0, 0, 1, 2, 0, 0, 0, 1]]
    for corner in range(1, 8):
        source, tree_of, depth = [0] * 3, [0] * 3, [0] * 3
        for tree in range(3):
            flip = came_by(tree, corner)
            tree_of[flip] = tree
            at = corner
            while at:
                at ^= 1 << came_by(tree, at)
                depth[flip] += 1
        for flip in range(3):
            child = corner ^ (1 << flip)
            if child:
                (tree,) = [t for t in range(3) if came_by(t, child) == flip]
                source[flip] = came_by(tree, corner)
        table.append(source + tree_of + depth + [0])
    return np.array(table, np.int32)


def corner_of(rank):
    turn = rank & 3
    return (rank >> 2) | ((((turn + 1) >> 1) & 1) << 1) | ((turn >> 1) << 2)


def own_plan(owner_rank):
    corner = corner_of(lax.axis_index("rep")) ^ corner_of(owner_rank)
    hot = (jnp.arange(8, dtype=jnp.int32) == corner).astype(jnp.int32)
    return jnp.sum(hot[:, None] * jnp.asarray(plan()), axis=0)


def exchange(sends):
    ranks = range(lax.axis_size("rep"))
    return [
        lax.ppermute(send, "rep", [(i, i ^ mask) for i in ranks])
        for send, mask in zip(sends, FLIPS)
    ]


def in_vmem(values):
    return [pltpu.with_memory_space_constraint(value, pltpu.VMEM) for value in values]


def piece_of(ref, index, columns=None):
    rows = pl.ds(pl.multiple_of(index * PIECE, PIECE), PIECE)
    return ref.at[rows, :] if columns is None else ref.at[rows, columns]


def visit(piece, arrays, act):
    block = piece // PER_BLOCK
    row = pl.multiple_of((piece % PER_BLOCK) * PIECE, PIECE)
    for quarter in range(4):

        @pl.when(block == quarter)
        def _():
            act(arrays[0].at[pl.ds(row, PIECE), pl.ds(512 * quarter, 512)], None)

    @pl.when((block >= 4) & (block < 8))
    def _():
        start = pl.multiple_of((piece - 4 * PER_BLOCK) * PIECE, PIECE)
        act(arrays[1].at[pl.ds(start, PIECE), :], None)

    for which in (2, 3):

        @pl.when(block == which + 6)
        def _():
            for quarter in range(4):
                start = pl.multiple_of(512 * quarter + row, PIECE)
                act(arrays[which].at[pl.ds(start, PIECE), :], pl.ds(128 * quarter, 128))


def forward(step, table, received, weights):
    relays, loads = received is not None, step < CHUNKS
    bases = [(step * 3 + flip) * PIECES for flip in range(3)]
    counts = [max(0, min(PIECES, TOTAL - base)) for base in bases]

    def kernel(*refs):
        refs = list(refs)
        table = refs.pop(0)
        came = [refs.pop(0) for _ in range(3)] if relays else None
        sources = [refs.pop(0) for _ in range(4)] if loads else None
        sends, sem = refs[:3], refs[3]
        is_owner = table[9] == 1
        if loads:

            @pl.when(is_owner)
            def _():
                for flip in range(3):

                    def begin(index, _):
                        visit(
                            bases[flip] + index,
                            sources,
                            lambda part, columns: pltpu.make_async_copy(
                                part, piece_of(sends[flip], index, columns), sem
                            ).start(),
                        )
                        return 0

                    lax.fori_loop(0, counts[flip], begin, 0)
                for flip in range(3):
                    if counts[flip]:
                        whole = sends[flip].at[pl.ds(0, counts[flip] * PIECE), :]
                        pltpu.make_async_copy(whole, whole, sem).wait()

        if relays:

            @pl.when(jnp.logical_not(is_owner))
            def _():
                for flip in range(3):
                    for source in range(3):

                        @pl.when(table[flip] == source)
                        def _():
                            for row in range(0, ROWS, 32):
                                sends[flip][row : row + 32, :] = came[source][row : row + 32, :]

    return pl.pallas_call(
        kernel,
        out_shape=[pltpu.VMEM((ROWS, WIDTH), jnp.bfloat16)] * 3,
        in_specs=[IN_SMEM] + [IN_VMEM] * (3 * relays) + [IN_HBM] * (4 * loads),
        out_specs=[IN_VMEM] * 3,
        scratch_shapes=[pltpu.SemaphoreType.DMA],
        compiler_params=pltpu.CompilerParams(vmem_limit_bytes=GRANT),
        name="forward",
    )(table, *(in_vmem(received) if relays else []), *(weights if loads else []))


def store(step, table, received, targets):
    def kernel(*refs):
        table, came, outs, sem = refs[0], refs[1:4], refs[8:12], refs[12]

        @pl.when(table[9] != 1)
        def _():
            counts = []
            for flip in range(3):
                chunk = step - (table[6 + flip] - 1)
                base = (chunk * 3 + table[3 + flip]) * PIECES
                count = jnp.where(
                    (chunk >= 0) & (chunk < CHUNKS), jnp.clip(TOTAL - base, 0, PIECES), 0
                )
                counts.append(count)

                def begin(index, _):
                    visit(
                        base + index,
                        outs,
                        lambda part, columns: pltpu.make_async_copy(
                            piece_of(came[flip], index, columns), part, sem
                        ).start(),
                    )
                    return 0

                lax.fori_loop(0, count, begin, 0)
            for flip in range(3):

                def finish(index, _):
                    whole = piece_of(came[flip], index)
                    pltpu.make_async_copy(whole, whole, sem).wait()
                    return 0

                lax.fori_loop(0, counts[flip], finish, 0)

    return pl.pallas_call(
        kernel,
        out_shape=[jax.ShapeDtypeStruct(target.shape, target.dtype) for target in targets],
        in_specs=[IN_SMEM] + [IN_VMEM] * 3 + [IN_HBM] * 4,
        out_specs=[IN_HBM] * 4,
        scratch_shapes=[pltpu.SemaphoreType.DMA],
        input_output_aliases={4 + k: k for k in range(4)},
        compiler_params=pltpu.CompilerParams(vmem_limit_bytes=GRANT),
        name="store",
    )(table, *in_vmem(received), *targets)


def cut_along(shard, dim, peers):
    lengths = shard.shape
    parts = shard.reshape(*lengths[:dim], peers, lengths[dim] // peers, *lengths[dim + 1 :])
    return jnp.moveaxis(parts, dim, 0)


def sent_and_summed(shard, axis, dim):
    peers = lax.axis_size(axis)
    parts = lax.all_to_all(cut_along(shard, dim, peers), axis, 0, 0, tiled=True)
    return jnp.sum(parts, axis=0)


def copy_for_each(shard, axis):
    peers = lax.axis_size(axis)
    return lax.all_to_all(
        jnp.broadcast_to(shard[None], (peers, *shard.shape)), axis, 0, 0, tiled=True
    )


def joined_along(parts, dim):
    parts = jnp.moveaxis(parts, 0, dim)
    lengths = parts.shape
    return parts.reshape(*lengths[:dim], lengths[dim] * lengths[dim + 1], *lengths[dim + 2 :])


def collect(shard, axis, dim):
    parts = copy_for_each(shard, axis)
    return joined_along(parts, dim)


def rotate(heads, positions):
    half_dim = heads.shape[-1] // 2
    frequency = rope_base ** (-(jnp.arange(half_dim, dtype=jnp.float32) * 2.0 / heads.shape[-1]))
    angles = positions.astype(jnp.float32)[:, None] * frequency[None, :]
    cosine = jnp.cos(angles)[:, None, :]
    sine_part = jnp.sin(angles)[:, None, :]
    first_half = heads[..., :half_dim]
    second_half = heads[..., half_dim:]
    return jnp.concatenate(
        [
            first_half * cosine - second_half * sine_part,
            second_half * cosine + first_half * sine_part,
        ],
        axis=-1,
    )


def attend(query, own_key, own_value, cache_key, cache_value, lengths):
    seqs, span, width = cache_key.shape
    kv_local = query.shape[1]
    head_size = query.shape[3]
    keys_view = cache_key.reshape(seqs, span, kv_local, head_size)
    values_view = cache_value.reshape(seqs, span, kv_local, head_size)
    scale = head_size ** (-0.5)
    scores = (
        jnp.einsum("shgd,sthd->shgt", query, keys_view, preferred_element_type=jnp.float32) * scale
    )
    own_score = (
        jnp.einsum("shgd,shd->shg", query, own_key, preferred_element_type=jnp.float32) * scale
    )
    live = (jnp.arange(span, dtype=jnp.int32)[None, :] < lengths[:, None])[:, None, None, :]
    masked = jnp.where(live, scores, -jnp.inf)
    row_max = jnp.maximum(jnp.max(masked, axis=-1), own_score)
    weights = jnp.where(live, jnp.exp(scores - row_max[..., None]), 0.0)
    own_weight = jnp.exp(own_score - row_max)
    denominator = jnp.sum(weights, axis=-1) + own_weight
    probs = (weights / denominator[..., None]).astype(jnp.bfloat16)
    own_prob = (own_weight / denominator).astype(jnp.bfloat16)
    context = jnp.einsum("shgt,sthd->shgd", probs, values_view, preferred_element_type=jnp.float32)
    return (
        context
        + own_prob.astype(jnp.float32)[..., None] * own_value.astype(jnp.float32)[:, :, None, :]
    )


def from_owner(parts, owner_rank):
    peers = lax.axis_size("rep")
    grouped = parts.reshape(peers, parts.shape[0] // peers, *parts.shape[1:])
    return lax.dynamic_index_in_dim(grouped, owner_rank, 0, keepdims=False)


def chain(
    hidden,
    cache_key,
    cache_value,
    lengths,
    owner,
    query_weight,
    key_weight,
    value_weight,
    out_weight,
):
    reps, fss, tps = lax.axis_size("rep"), lax.axis_size("fs"), lax.axis_size("tp")
    owner_rank = owner[0] % reps
    hidden = yield hidden
    seqs = hidden.shape[0]
    hidden_wide = collect(hidden, "tp", 1).astype(jnp.float32)
    normed = (
        hidden_wide
        * lax.rsqrt(jnp.mean(hidden_wide * hidden_wide, axis=-1, keepdims=True) + epsilon)
    ).astype(jnp.bfloat16)
    blocks = cut_along(normed, 1, fss)
    blocks = jnp.broadcast_to(blocks[None], (reps, *blocks.shape))
    blocks = blocks.reshape(reps * fss, *blocks.shape[2:])
    blocks = yield blocks
    tokens = lax.all_to_all(blocks, ("rep", "fs"), 0, 0, tiled=True)
    tokens = tokens.reshape(reps * fss * seqs, tokens.shape[-1])
    tokens = yield tokens
    query_width = query_weight.shape[2]
    key_width = key_weight.shape[2]
    partial = jnp.concatenate(
        [
            jnp.dot(tokens, query_weight[0], preferred_element_type=jnp.float32),
            jnp.dot(tokens, key_weight[0], preferred_element_type=jnp.float32),
            jnp.dot(tokens, value_weight[0], preferred_element_type=jnp.float32),
        ],
        axis=1,
    )
    partial = partial.reshape(reps * fss, seqs, partial.shape[1])
    shares = lax.all_to_all(partial, ("rep", "fs"), 0, 0, tiled=True)
    shares = yield shares
    joined = jnp.sum(from_owner(shares, owner_rank), axis=0)
    query_proj = joined[:, :query_width]
    key_proj = joined[:, query_width : query_width + key_width]
    value_proj = joined[:, query_width + key_width :]
    q_heads = query_proj.shape[1] // DH
    kv_heads = key_proj.shape[1] // DH
    query_rot = rotate(query_proj.reshape(seqs, q_heads, DH), lengths).astype(jnp.bfloat16)
    query_rot = query_rot.reshape(seqs, kv_heads, q_heads // kv_heads, DH)
    key_new = rotate(key_proj.reshape(seqs, kv_heads, DH), lengths).astype(jnp.bfloat16)
    value_new = value_proj.astype(jnp.bfloat16).reshape(seqs, kv_heads, DH)
    context = attend(query_rot, key_new, value_new, cache_key, cache_value, lengths)
    context = context.astype(jnp.bfloat16).reshape(seqs, q_heads * DH)
    contexts = lax.all_to_all(
        jnp.broadcast_to(context[None], (reps * fss, *context.shape)), ("rep", "fs"), 0, 0, tiled=True
    ).reshape(reps * fss * seqs, q_heads * DH)
    contexts = yield contexts
    partial_out = jnp.dot(contexts, out_weight[0], preferred_element_type=jnp.float32)
    partial_out = partial_out.reshape(reps * fss, seqs, partial_out.shape[1])
    terms = lax.all_to_all(partial_out, ("rep", "fs"), 0, 0, tiled=True)
    terms = joined_along(from_owner(terms, owner_rank), 1)
    terms = yield terms
    summed = sent_and_summed(terms, "tp", 1)
    mixed = (summed + hidden.astype(jnp.float32)).astype(jnp.bfloat16)
    return (
        mixed,
        key_new.reshape(seqs, kv_heads * DH),
        value_new.reshape(seqs, kv_heads * DH),
    )


def local(*arguments):
    owner_rank = arguments[4][0] % lax.axis_size("rep")
    query_weight, key_weight, value_weight, out_weight = [weight[0] for weight in arguments[5:]]
    weights = [out_weight, query_weight, key_weight, value_weight]
    table = own_plan(owner_rank)
    work = chain(*arguments)
    waiting, results = next(work), None
    received, targets = None, weights
    for step in range(ROUNDS):
        sends = forward(step, table, received, weights)
        if received is None:
            sends, waiting = lax.optimization_barrier((sends, waiting))
        else:
            sends, received, waiting = lax.optimization_barrier((sends, received, waiting))
            targets = store(step - 1, table, received, targets)
        received = exchange(sends)
        try:
            if results is None:
                waiting = work.send(waiting)
        except StopIteration as end:
            results, waiting = end.value, ()
        received, targets = lax.optimization_barrier((received, targets))
    targets = store(ROUNDS - 1, table, received, targets)
    fresh_out, fresh_query, fresh_key, fresh_value = [target[None] for target in targets]
    return (*results, fresh_query, fresh_key, fresh_value, fresh_out)


def solution(mesh):
    return jax.shard_map(
        local,
        mesh=mesh,
        in_specs=(
            P(("rep", "fs"), "tp"),
            P(("rep", "fs"), None, "tp"),
            P(("rep", "fs"), None, "tp"),
            P(("rep", "fs")),
            P(),
            P("rep", "fs", "tp"),
            P("rep", "fs", "tp"),
            P("rep", "fs", "tp"),
            P("rep", "tp", "fs"),
        ),
        out_specs=(
            P(("rep", "fs"), "tp"),
            P(("rep", "fs"), "tp"),
            P(("rep", "fs"), "tp"),
            P("rep", "fs", "tp"),
            P("rep", "fs", "tp"),
            P("rep", "fs", "tp"),
            P("rep", "tp", "fs"),
        ),
        check_vma=False,
    )
```
